128 devices in a mesh: data: 1, group: 128 (over z, y, x, core).
Axes of the slice: x: 4, y: 4, z: 4, core: 2. Of those that a mesh axis runs over, the one named last changes fastest.
Arguments:
- latents: bfloat16 [2048, 768], P(('data', 'group'))
- hint_embed: bfloat16 [2048, 768], P(('data', 'group'))
- in_qkv: bfloat16 [2, 9, 768, 2304], replicated
- in_proj: bfloat16 [2, 9, 12, 64, 768], replicated
- in_up: bfloat16 [2, 9, 768, 3072], replicated
- in_down: bfloat16 [2, 9, 3072, 768], replicated
- in_norm: bfloat16 [2, 9, 4, 768], replicated
- out_qkv: bfloat16 [8, 768, 2304], replicated
- out_proj: bfloat16 [8, 12, 64, 768], replicated
- out_up: bfloat16 [8, 768, 3072], replicated
- out_down: bfloat16 [8, 3072, 768], replicated
- out_norm: bfloat16 [8, 4, 768], replicated
- zero_proj: bfloat16 [9, 768, 768], replicated
- hint_proj: bfloat16 [768, 768], replicated
- skip_proj: bfloat16 [8, 1536, 768], replicated
- final_norm: bfloat16 [2, 768], replicated
- w_out: bfloat16 [768, 768], replicated
Outputs:
- output: bfloat16 [2048, 768], P(('data', 'group'))
All inputs are finite; a program needn't handle non-finite values.
Results may differ from the reference program's by a relative error of at most 0.02.
Values are sent between devices in bfloat16 or wider.
A program may use at most 1.5 GiB of HBM per device.

```python
import math
import jax
import jax.numpy as jnp
from jax import lax

TOKENS = 2048
WIDTH = 768
HEADS = 12
LAYERS = 8

HEAD_DIM = WIDTH // HEADS
IN_BLOCKS = LAYERS + 1
Q_GAIN = math.sqrt(max(1.0, math.log(TOKENS / 16.0)))
EPS = 1e-6


def draw_normal(rng_key, dim_sizes, std_scale):
    return (jax.random.normal(rng_key, dim_sizes, jnp.float32) * std_scale).astype(jnp.bfloat16)


def draw_qkv(rng_key, lead_dims):
    col_gain = jnp.concatenate([jnp.full((WIDTH,), Q_GAIN, jnp.float32), jnp.ones((2 * WIDTH,), jnp.float32)])
    raw_vals = jax.random.normal(rng_key, lead_dims + (WIDTH, 3 * WIDTH), jnp.float32)
    return (raw_vals * col_gain * WIDTH ** -0.5).astype(jnp.bfloat16)


def draw_norms(rng_key, lead_dims, row_count):
    centre = jnp.tile(jnp.array([1.0, 0.0], jnp.float32), row_count // 2)[:, None]
    raw_vals = jax.random.normal(rng_key, lead_dims + (row_count, WIDTH), jnp.float32)
    return (raw_vals * 0.2 + centre).astype(jnp.bfloat16)


def setup_inputs(seed: int = 0, part: int = 0) -> dict:
    part_keys = jax.random.split(jax.random.fold_in(jax.random.key(seed), part), 2)
    rng_keys = jax.random.split(jax.random.key(seed + 1), 15)
    in_lead = (2, IN_BLOCKS)
    out_lead = (LAYERS,)
    return {
        "latents": draw_normal(part_keys[0], (TOKENS, WIDTH), 1.0),
        "hint_embed": draw_normal(part_keys[1], (TOKENS, WIDTH), 1.0),
        "in_qkv": draw_qkv(rng_keys[0], in_lead),
        "in_proj": draw_normal(rng_keys[1], in_lead + (HEADS, HEAD_DIM, WIDTH), WIDTH ** -0.5),
        "in_up": draw_normal(rng_keys[2], in_lead + (WIDTH, 4 * WIDTH), WIDTH ** -0.5),
        "in_down": draw_normal(rng_keys[3], in_lead + (4 * WIDTH, WIDTH), (4 * WIDTH) ** -0.5),
        "in_norm": draw_norms(rng_keys[4], in_lead, 4),
        "out_qkv": draw_qkv(rng_keys[5], out_lead),
        "out_proj": draw_normal(rng_keys[6], out_lead + (HEADS, HEAD_DIM, WIDTH), WIDTH ** -0.5),
        "out_up": draw_normal(rng_keys[7], out_lead + (WIDTH, 4 * WIDTH), WIDTH ** -0.5),
        "out_down": draw_normal(rng_keys[8], out_lead + (4 * WIDTH, WIDTH), (4 * WIDTH) ** -0.5),
        "out_norm": draw_norms(rng_keys[9], out_lead, 4),
        "zero_proj": draw_normal(rng_keys[10], (IN_BLOCKS, WIDTH, WIDTH), 0.6 * WIDTH ** -0.5),
        "hint_proj": draw_normal(rng_keys[11], (WIDTH, WIDTH), WIDTH ** -0.5),
        "skip_proj": draw_normal(rng_keys[12], (LAYERS, 2 * WIDTH, WIDTH), (2 * WIDTH) ** -0.5),
        "final_norm": draw_norms(rng_keys[13], (), 2),
        "w_out": draw_normal(rng_keys[14], (WIDTH, WIDTH), WIDTH ** -0.5),
    }


def mat_f32(left_op, right_op):
    return jnp.dot(left_op, right_op, preferred_element_type=jnp.float32)


def layer_norm(values, norm_gain, norm_shift):
    wide_vals = values.astype(jnp.float32)
    centered = wide_vals - jnp.mean(wide_vals, axis=-1, keepdims=True)
    variance = jnp.mean(centered * centered, axis=-1, keepdims=True)
    normed = centered * lax.rsqrt(variance + EPS)
    return (normed * norm_gain.astype(jnp.float32) + norm_shift.astype(jnp.float32)).astype(jnp.bfloat16)


def head_attend(head_args):
    queries, key_rows, val_rows = head_args
    scores = mat_f32(queries, key_rows.T) * HEAD_DIM ** -0.5
    att_probs = jax.nn.softmax(scores, axis=-1).astype(jnp.bfloat16)
    return mat_f32(att_probs, val_rows).astype(jnp.bfloat16)


def transformer_block(residual, params):
    w_qkv, w_proj, w_up, w_down, norm_rows = params
    normed = layer_norm(residual, norm_rows[0], norm_rows[1])
    qkv_all = mat_f32(normed, w_qkv).astype(jnp.bfloat16)
    by_head = qkv_all.reshape(TOKENS, 3, HEADS, HEAD_DIM).transpose(1, 2, 0, 3)
    head_out = lax.map(head_attend, (by_head[0], by_head[1], by_head[2]))
    head_out = head_out.transpose(1, 0, 2).reshape(TOKENS, WIDTH)
    residual = (residual.astype(jnp.float32) + mat_f32(head_out, w_proj.reshape(WIDTH, WIDTH))).astype(jnp.bfloat16)
    normed = layer_norm(residual, norm_rows[2], norm_rows[3])
    hidden = jax.nn.gelu(mat_f32(normed, w_up), approximate=True).astype(jnp.bfloat16)
    return (residual.astype(jnp.float32) + mat_f32(hidden, w_down)).astype(jnp.bfloat16)


def reference(latents, hint_embed, in_qkv, in_proj, in_up, in_down, in_norm, out_qkv, out_proj, out_up, out_down, out_norm, zero_proj, hint_proj, skip_proj, final_norm, w_out):
    def in_step(residual, params):
        residual = transformer_block(residual, params)
        return residual, residual

    def out_step(residual, xs_pack):
        merged = mat_f32(jnp.concatenate([residual, xs_pack[6]], axis=-1), xs_pack[5]).astype(jnp.bfloat16)
        return transformer_block(merged, xs_pack[:5]), None

    ctrl_start = (latents.astype(jnp.float32) + mat_f32(hint_embed, hint_proj)).astype(jnp.bfloat16)
    base_params = (in_qkv[0], in_proj[0], in_up[0], in_down[0], in_norm[0])
    ctrl_params = (in_qkv[1], in_proj[1], in_up[1], in_down[1], in_norm[1])
    base_outs = lax.scan(in_step, latents, base_params)[1]
    ctrl_outs = lax.scan(in_step, ctrl_start, ctrl_params)[1]
    ctrl_res = jnp.einsum("bnd,bde->bne", ctrl_outs.astype(jnp.float32), zero_proj.astype(jnp.float32)).astype(jnp.bfloat16)
    sum_all = (base_outs.astype(jnp.float32) + ctrl_res.astype(jnp.float32)).astype(jnp.bfloat16)
    out_xs = (out_qkv, out_proj, out_up, out_down, out_norm, skip_proj, sum_all[:LAYERS][::-1])
    out_state = lax.scan(out_step, sum_all[LAYERS], out_xs)[0]
    normed = layer_norm(out_state, final_norm[0], final_norm[1])
    return mat_f32(normed, w_out).astype(jnp.bfloat16)
```

```python
import functools

import jax
import jax.numpy as jnp
from jax import lax
from jax.experimental import pallas as pl
from jax.experimental.pallas import tpu as pltpu
from jax.sharding import PartitionSpec as P

EPS = 1e-6
MESH = pl.DeviceIdType.MESH
LOG2E = 1.4426950408889634
ROWS = 32
HALF_ROWS = 16


def mat_f32(left_op, right_op):
    return jnp.dot(left_op, right_op, preferred_element_type=jnp.float32)


def layer_norm(values, gain, shift):
    wide_vals = values.astype(jnp.float32)
    centered = wide_vals - jnp.mean(wide_vals, axis=-1, keepdims=True)
    variance = jnp.mean(centered * centered, axis=-1, keepdims=True)
    normed = centered * lax.rsqrt(variance + EPS)
    return (normed * gain.astype(jnp.float32) + shift.astype(jnp.float32)).astype(jnp.bfloat16)


def gelu(v):
    inner = 0.7978845608028654 * (v + 0.044715 * (v * v * v))
    return 0.5 * v * (1.0 + jnp.tanh(inner))


def stack_kernel(n_blocks, two_branch, has_skip, *refs):
    if has_skip:
        x_ref, s_ref, norm_ref, skip_hbm, qkv_hbm, proj_hbm, up_hbm, down_hbm, out_ref, *scratch = refs
        (w_skip, *scratch) = scratch
    else:
        x_ref, norm_ref, qkv_hbm, proj_hbm, up_hbm, down_hbm, out_ref, *scratch = refs
    (t_all, w_qkv, w_proj, w_up, w_down, v_buf, s_buf, m_buf, a_buf, a_full, u_buf,
     w_sem, p1, p2, p3, s1, s2, s3, a_recv, q1, q2, q3, f1, f2, f3, a_send) = scratch
    width = x_ref.shape[-1]
    half_w = width // 2
    hid = w_up.shape[-1]

    data_idx = lax.axis_index("data")
    me = lax.axis_index("group")
    core = lax.rem(me, 2)
    chip = me // 2
    x_pos = lax.rem(chip, 4)
    y_pos = lax.rem(chip // 4, 4)
    z_full = chip // 16
    half = z_full // 2
    z_pos = lax.rem(z_full, 2)
    sib_core = 1 - core
    sibling = me + 1 - 2 * core

    def dev(zz, yy, xx):
        return (((half * 2 + zz) * 4 + yy) * 4 + xx) * 2 + core

    def shift(pos, d):
        return lax.rem(pos + d + 4, 4)

    def z_of(dz):
        return z_pos if dz == 0 else 1 - z_pos

    relay = (y_pos, x_pos)

    def group(par, k, cc, zz, r):
        if k == 0:
            return t_all.at[par, cc, zz, r, :, pl.ds(0, HALF_ROWS), :]
        return t_all.at[par, cc, zz, :, r, pl.ds(HALF_ROWS, HALF_ROWS), :]

    def piece(par, k, zz, yy, xx):
        return t_all.at[par, core, zz, yy, xx, pl.ds(k * HALF_ROWS, HALF_ROWS), :]

    def remote(region, target, send_sem, recv_sem):
        return pltpu.make_async_remote_copy(
            src_ref=region, dst_ref=region, send_sem=send_sem, recv_sem=recv_sem,
            device_id=(data_idx, target), device_id_type=MESH)

    def leg1(par, k, dz, d, receive=False):
        sems = (q1.at[k, dz, d], p1.at[par, k, dz, d])
        if receive:
            src = (z_of(dz), y_pos, shift(x_pos, -d)) if k == 0 else (z_of(dz), shift(y_pos, -d), x_pos)
            return remote(piece(par, k, *src), dev(*src), *sems)
        dst = (z_of(dz), y_pos, shift(x_pos, d)) if k == 0 else (z_of(dz), shift(y_pos, d), x_pos)
        return remote(piece(par, k, z_pos, y_pos, x_pos), dev(*dst), *sems)

    def along(k, d):
        return dev(z_pos, shift(y_pos, d), x_pos) if k == 0 else dev(z_pos, y_pos, shift(x_pos, d))

    step_of = (1, -1)

    def leg2(par, k, dz, way, receive=False):
        sems = (q2.at[k, dz, way], p2.at[par, k, dz, way])
        d = step_of[way]
        at = shift(relay[k], -d) if receive else relay[k]
        return remote(group(par, k, core, z_of(dz), at), along(k, d), *sems)

    def leg3(par, k, way, receive=False):
        sems = (q3.at[k, way], p3.at[par, k, way])
        d = step_of[way]
        at = shift(relay[k], -2 * d) if receive else shift(relay[k], -d)
        return remote(group(par, k, core, z_of(way), at), along(k, d), *sems)

    def side1(par, k, dz, cc):
        return remote(group(par, k, cc, z_of(dz), relay[k]), sibling, f1.at[k, dz], s1.at[par, k, dz])

    def side2(par, k, dz, way, cc):
        region = group(par, k, cc, z_of(dz), shift(relay[k], -step_of[way]))
        return remote(region, sibling, f2.at[k, dz, way], s2.at[par, k, dz, way])

    def side3(par, k, way, cc):
        region = group(par, k, cc, z_of(way), shift(relay[k], 2))
        return remote(region, sibling, f3.at[k, way], s3.at[par, k, way])

    leg1_keys = [(k, dz, d) for dz, d in ((1, 2), (0, 2), (1, 1), (1, 3), (0, 1), (0, 3), (1, 0)) for k in (0, 1)]

    def layer_of(ref, i):
        return ref.at[half, i] if two_branch else ref.at[i]

    def qkv_copies(i):
        cols = lambda part: pl.ds(pl.multiple_of(part * width + core * half_w, 128), half_w)
        return [pltpu.make_async_copy(layer_of(qkv_hbm, i).at[:, cols(p)], w_qkv.at[:, pl.ds(p * half_w, half_w)], w_sem.at[p]) for p in range(3)]

    def proj_copies(i):
        return [pltpu.make_async_copy(layer_of(proj_hbm, i), w_proj, w_sem.at[3])]

    def up_copies(i):
        return [pltpu.make_async_copy(layer_of(up_hbm, i), w_up, w_sem.at[4])]

    def down_copies(i):
        return [pltpu.make_async_copy(layer_of(down_hbm, i), w_down, w_sem.at[5])]

    def skip_copies(i):
        return [pltpu.make_async_copy(skip_hbm.at[i], w_skip, w_sem.at[6])]

    def start(copies):
        for c in copies:
            c.start()

    def wait(copies):
        for c in copies:
            c.wait()

    def start_next(make, i):
        @pl.when(i + 1 < n_blocks)
        def _():
            start(make(i + 1))

    if has_skip:
        start(skip_copies(0))
    for make in (qkv_copies, proj_copies, up_copies, down_copies):
        start(make(0))
    u_buf[...] = x_ref[...]

    lane = lax.broadcasted_iota(jnp.int32, (2 * ROWS, 128), 1)

    def block(i, carry):
        par = lax.rem(i, 2)
        if has_skip:
            wait(skip_copies(i))
            merged = mat_f32(u_buf[...], w_skip[0:width, :]) + mat_f32(s_ref[i], w_skip[width:2 * width, :])
            u_buf[...] = merged.astype(jnp.bfloat16)
            start_next(skip_copies, i)
        t = layer_norm(u_buf[...], norm_ref[i, 0:1, :], norm_ref[i, 1:2, :])
        t_all[par, core, z_pos, y_pos, x_pos] = t
        for key in leg1_keys:
            leg1(par, *key).start()

        for dz in (0, 1):
            for k in (0, 1):
                for d in range(4):
                    if dz or d:
                        leg1(par, k, dz, d, receive=True).wait_recv()
                leg2(par, k, dz, 0).start()
                leg2(par, k, dz, 1).start()
                side1(par, k, dz, core).start()

        wait(qkv_copies(i))

        def chunk(j, k, r):
            rows = []
            for cc in range(2):
                for zz in range(2):
                    for o in range(4):
                        if k == 0:
                            rows.append(t_all[par, cc, zz, r, o, 0:HALF_ROWS, :])
                        else:
                            rows.append(t_all[par, cc, zz, o, r, HALF_ROWS:ROWS, :])
            toks = jnp.concatenate(rows, axis=0)
            n = toks.shape[0]
            kv = mat_f32(toks, w_qkv[:, half_w:3 * half_w]).astype(jnp.bfloat16)
            v_buf[j * n:(j + 1) * n, :] = kv[:, half_w:]
            for p in range(3):
                sc = lax.dot_general(q_bd[p], kv[:, p * 128:(p + 1) * 128], (((1,), (1,)), ((), ())), preferred_element_type=jnp.float32)
                s_buf[p, :, j * n:(j + 1) * n] = sc
                top = jnp.maximum(sc[:, 0:128], sc[:, 128:256])
                m_buf[p] = top if j == 0 else jnp.maximum(m_buf[p], top)

        for dz in (0, 1):
            for k in (0, 1):
                side1(par, k, dz, sib_core).wait_recv()
        own = jnp.concatenate([t_all[par, 0, z_pos, y_pos, x_pos], t_all[par, 1, z_pos, y_pos, x_pos]], axis=0)
        q = mat_f32(own, w_qkv[:, 0:half_w])
        q_bd = []
        for p in range(3):
            qp = q[:, p * 128:(p + 1) * 128]
            q_bd.append(jnp.concatenate([jnp.where(lane < 64, qp, 0.0), jnp.where(lane < 64, 0.0, qp)], axis=0).astype(jnp.bfloat16))

        chunk(0, 0, relay[0])

        def take2(k, dz, way, forward):
            leg2(par, k, dz, way, receive=True).wait_recv()
            if forward:
                leg3(par, k, way).start()
            side2(par, k, dz, way, core).start()

        take2(0, 0, 0, True)
        take2(1, 0, 0, True)
        chunk(1, 1, relay[1])
        take2(0, 1, 1, True)
        take2(1, 1, 1, True)
        for k in (0, 1):
            take2(k, 1, 0, False)
            take2(k, 0, 1, False)
        j = 2
        for k in (0, 1):
            for way in (0, 1):
                for dz in (0, 1):
                    side2(par, k, dz, way, sib_core).wait_recv()
                chunk(j, k, shift(relay[k], -step_of[way]))
                j += 1
        for k in (0, 1):
            for way in (0, 1):
                leg3(par, k, way, receive=True).wait_recv()
                side3(par, k, way, core).start()
        for k in (0, 1):
            for way in (0, 1):
                side3(par, k, way, sib_core).wait_recv()
            chunk(j, k, shift(relay[k], 2))
            j += 1
        start_next(qkv_copies, i)

        n_chunks, n = 8, 256
        scale = 64 ** -0.5 * LOG2E
        for p in range(3):
            top = jnp.max(m_buf[p], axis=-1, keepdims=True)
            part = None
            for j in range(n_chunks):
                e = jnp.exp2((s_buf[p, :, j * n:(j + 1) * n] - top) * scale)
                s_buf[p, :, j * n:(j + 1) * n] = e
                both = e[:, 0:128] + e[:, 128:256]
                part = both if part is None else part + both
            inv = 1.0 / jnp.sum(part, axis=-1, keepdims=True)
            acc = None
            for j in range(n_chunks):
                pr = (s_buf[p, :, j * n:(j + 1) * n] * inv).astype(jnp.bfloat16)
                o = mat_f32(pr, v_buf[j * n:(j + 1) * n, p * 128:(p + 1) * 128])
                acc = o if acc is None else acc + o
            a = jnp.where(lane < 64, acc[0:2 * ROWS], acc[2 * ROWS:4 * ROWS]).astype(jnp.bfloat16)
            a_buf[0, :, p * 128:(p + 1) * 128] = a[0:ROWS]
            a_buf[1, :, p * 128:(p + 1) * 128] = a[ROWS:2 * ROWS]

        swap = pltpu.make_async_remote_copy(
            src_ref=a_buf.at[sib_core], dst_ref=a_full.at[core], send_sem=a_send, recv_sem=a_recv,
            device_id=(data_idx, sibling), device_id_type=MESH)
        swap.start()
        a_full[core] = a_buf[core]
        swap.wait_send()
        pltpu.make_async_remote_copy(
            src_ref=a_buf.at[core], dst_ref=a_full.at[sib_core], send_sem=a_send, recv_sem=a_recv,
            device_id=(data_idx, sibling), device_id_type=MESH).wait_recv()

        wait(proj_copies(i))
        attn = mat_f32(a_full[0], w_proj[0:half_w, :]) + mat_f32(a_full[1], w_proj[half_w:width, :])
        start_next(proj_copies, i)
        mid = (u_buf[...].astype(jnp.float32) + attn).astype(jnp.bfloat16)
        t2 = layer_norm(mid, norm_ref[i, 2:3, :], norm_ref[i, 3:4, :])
        wait(up_copies(i))
        wait(down_copies(i))
        acc = None
        for c in range(0, hid, width):
            h = gelu(mat_f32(t2, w_up[:, c:c + width])).astype(jnp.bfloat16)
            o = mat_f32(h, w_down[c:c + width, :])
            acc = o if acc is None else acc + o
        start_next(up_copies, i)
        start_next(down_copies, i)
        res = (mid.astype(jnp.float32) + acc).astype(jnp.bfloat16)
        u_buf[...] = res
        if not has_skip:
            out_ref[i] = res

        for key in leg1_keys:
            leg1(par, *key).wait_send()
        for k in (0, 1):
            for way in (0, 1):
                for dz in (0, 1):
                    leg2(par, k, dz, way).wait_send()
                    side2(par, k, dz, way, core).wait_send()
                leg3(par, k, way).wait_send()
                side3(par, k, way, core).wait_send()
            for dz in (0, 1):
                side1(par, k, dz, core).wait_send()
        return carry

    lax.fori_loop(0, n_blocks, block, 0)
    if has_skip:
        out_ref[...] = u_buf[...]


def run_stack(x, norm, qkv, proj, up, down, skip=None, s=None):
    two_branch = qkv.ndim == 4
    has_skip = skip is not None
    n_blocks, width, hid = norm.shape[0], x.shape[-1], up.shape[-1]
    vmem, hbm = pl.BlockSpec(memory_space=pltpu.VMEM), pl.BlockSpec(memory_space=pl.ANY)
    bf, f32, dma = jnp.bfloat16, jnp.float32, pltpu.SemaphoreType.DMA
    scratch = [
        pltpu.VMEM((2, 2, 2, 4, 4, ROWS, width), bf),
        pltpu.VMEM((width, 3 * width // 2), bf),
        pltpu.VMEM((width, width), bf),
        pltpu.VMEM((width, hid), bf),
        pltpu.VMEM((hid, width), bf),
        pltpu.VMEM((2048, width // 2), bf),
        pltpu.VMEM((3, 128, 2048), f32),
        pltpu.VMEM((3, 128, 128), f32),
        pltpu.VMEM((2, ROWS, width // 2), bf),
        pltpu.VMEM((2, ROWS, width // 2), bf),
        pltpu.VMEM((ROWS, width), bf),
        dma((7,)),
        dma((2, 2, 2, 4)), dma((2, 2, 2, 2)), dma((2, 2, 2)),
        dma((2, 2, 2)), dma((2, 2, 2, 2)), dma((2, 2, 2)), dma(()),
        dma((2, 2, 4)), dma((2, 2, 2)), dma((2, 2)),
        dma((2, 2)), dma((2, 2, 2)), dma((2, 2)), dma(()),
    ]
    if has_skip:
        scratch = [pltpu.VMEM((2 * width, width), bf)] + scratch
        args, specs = (x, s, norm, skip, qkv, proj, up, down), [vmem] * 3 + [hbm] * 5
        out = jax.ShapeDtypeStruct((ROWS, width), bf)
    else:
        args, specs = (x, norm, qkv, proj, up, down), [vmem] * 2 + [hbm] * 4
        out = jax.ShapeDtypeStruct((n_blocks, ROWS, width), bf)
    return pl.pallas_call(
        functools.partial(stack_kernel, n_blocks, two_branch, has_skip),
        out_shape=out, in_specs=specs, out_specs=vmem, scratch_shapes=scratch,
        name="out_stack" if has_skip else "in_stack",
        compiler_params=pltpu.CompilerParams(has_side_effects=True, vmem_limit_bytes=48 * 1024 * 1024),
    )(*args)


def solution(mesh):
    group_size = mesh.shape["group"]
    half_size = group_size // 2
    swap_perm = [(dev_id, (dev_id + half_size) % group_size) for dev_id in range(group_size)]
    to_base = [(dev_id + half_size, dev_id) for dev_id in range(half_size)]
    to_ctrl = [(dev_id, dev_id + half_size) for dev_id in range(half_size)]

    def device_step(x_own, hint_own, in_qkv, in_proj, in_up, in_down, in_norm, out_qkv, out_proj, out_up, out_down, out_norm, zero_proj, hint_proj, skip_proj, final_norm, w_out):
        layers = skip_proj.shape[0]
        tok_own, model_width = x_own.shape
        branch = lax.axis_index("group") // half_size
        is_base = branch == 0
        x_other = lax.ppermute(x_own, "group", swap_perm)
        hint_recv = lax.ppermute(hint_own, "group", to_ctrl)
        x_local = jnp.where(is_base, jnp.concatenate([x_own, x_other], axis=0), jnp.concatenate([x_other, x_own], axis=0))
        hint_local = jnp.where(is_base, jnp.zeros((2 * tok_own, model_width), jnp.bfloat16), jnp.concatenate([hint_recv, hint_own], axis=0))
        start = (x_local.astype(jnp.float32) + mat_f32(hint_local, hint_proj)).astype(jnp.bfloat16)
        flat = lambda w: w.reshape(w.shape[:-3] + (model_width, model_width))
        hist = run_stack(start, in_norm[branch].astype(jnp.float32), in_qkv, flat(in_proj), in_up, in_down)
        ctrl_res = jnp.einsum("lnd,lde->lne", hist, zero_proj, preferred_element_type=jnp.float32).astype(jnp.bfloat16)
        res_recv = lax.ppermute(ctrl_res, "group", to_base)
        sums = (hist.astype(jnp.float32) + res_recv.astype(jnp.float32)).astype(jnp.bfloat16)
        out_state = run_stack(sums[layers], out_norm.astype(jnp.float32), out_qkv, flat(out_proj), out_up, out_down, skip_proj, sums[:layers][::-1])
        normed = layer_norm(out_state, final_norm[0], final_norm[1])
        y_local = mat_f32(normed, w_out).astype(jnp.bfloat16)
        y_recv = lax.ppermute(y_local[tok_own:], "group", to_ctrl)
        return jnp.where(is_base, y_local[:tok_own], y_recv)

    tok_spec = P(("data", "group"), None)
    return jax.shard_map(device_step, mesh=mesh, in_specs=(tok_spec, tok_spec) + (P(),) * 15, out_specs=tok_spec, check_vma=False)
```

```python
import functools

import jax
import jax.numpy as jnp
from jax import lax
from jax.experimental import pallas as pl
from jax.experimental.pallas import tpu as pltpu
from jax.sharding import PartitionSpec as P

EPS = 1e-6
MESH = pl.DeviceIdType.MESH
SCALE = 64 ** -0.5 * 1.4426950408889634
ROWS = 32
SLAB = 16


def mat_f32(left_op, right_op):
    return jnp.dot(left_op, right_op, preferred_element_type=jnp.float32)


def layer_norm(values, gain, shift):
    wide_vals = values.astype(jnp.float32)
    centered = wide_vals - jnp.mean(wide_vals, axis=-1, keepdims=True)
    variance = jnp.mean(centered * centered, axis=-1, keepdims=True)
    normed = centered * lax.rsqrt(variance + EPS)
    return (normed * gain + shift).astype(jnp.bfloat16)


def gelu(v):
    inner = 0.7978845608028654 * (v + 0.044715 * (v * v * v))
    return 0.5 * v * (1.0 + jnp.tanh(inner))


def net_kernel(x_ref, hint_ref, in_norm, out_norm, final_norm, in_qkv, in_proj, in_up, in_down,
               out_qkv, out_proj, out_up, out_down, zero_hbm, hint_hbm, skip_hbm, wout_hbm, y_ref,
               t_all, w_qkv, w_proj, w_up, w_down, w_skip, w_sq, v_buf, s_buf, top_buf, sum_buf, a_buf, a_full,
               u_buf, xh_buf, hist, r_out, r_in, y_out, y_in,
               w_sem, p1, p2, s1, q1, q2, f1, a_recv, a_send, x_recv, x_send, r_recv, r_send, y_recv, y_send):
    n_in, n_out = in_norm.shape[1], out_norm.shape[0]
    width = x_ref.shape[-1]
    half_w = width // 2
    hid = w_up.shape[-1]

    data_idx = lax.axis_index("data")
    me = lax.axis_index("group")
    core = lax.rem(me, 2)
    chip = me // 2
    x_pos = lax.rem(chip, 4)
    y_pos = lax.rem(chip // 4, 4)
    z_full = chip // 16
    half = z_full // 2
    z_pos = lax.rem(z_full, 2)
    sib_core = 1 - core
    sibling = me + 1 - 2 * core
    partner = me + 64 - 128 * half
    r_pos = y_pos + core * (x_pos - y_pos)
    d_pos = x_pos + core * (y_pos - x_pos)

    def dev(zz, r, d):
        yy = r + core * (d - r)
        xx = d + core * (r - d)
        return (((half * 2 + zz) * 4 + yy) * 4 + xx) * 2 + core

    def shift(pos, d):
        return lax.rem(pos + d + 4, 4)

    def z_of(dz):
        return z_pos if dz == 0 else 1 - z_pos

    def send(src, dst, target, send_sem, recv_sem):
        return pltpu.make_async_remote_copy(
            src_ref=src, dst_ref=dst, send_sem=send_sem, recv_sem=recv_sem,
            device_id=(data_idx, target), device_id_type=MESH)

    def remote(region, target, send_sem, recv_sem):
        return send(region, region, target, send_sem, recv_sem)

    def leg1(par, dz, d, receive=False):
        sems = (q1.at[dz, d], p1.at[par, dz, d])
        if receive:
            return remote(t_all.at[par, core, z_of(dz), r_pos, shift(d_pos, -d)], sibling, *sems)
        return remote(t_all.at[par, core, z_pos, r_pos, d_pos], dev(z_of(dz), r_pos, shift(d_pos, d)), *sems)

    def onward(dz, d):
        return (dz + (d in (1, 2))) % 2

    def leg2(par, dz, d, way, receive=False):
        sems = (q2.at[dz, d, way], p2.at[par, dz, d, way])
        zz, dd = z_of(dz), shift(d_pos, -d)
        if way < 2:
            w = 1 - 2 * way
            at, to = (shift(r_pos, -w) if receive else r_pos), shift(r_pos, w)
        elif (dz, d) == (1, 2):
            at, to = (shift(r_pos, 2) if receive else r_pos), shift(r_pos, 2)
        else:
            w = 1 - 2 * onward(dz, d)
            at, to = shift(r_pos, 2 if receive else -w), shift(r_pos, w)
        return remote(t_all.at[par, core, zz, at, dd], dev(z_pos, to, d_pos), *sems)

    def side(par, dz, ro, cc):
        at = shift(r_pos if cc is core else d_pos, ro)
        return remote(t_all.at[par, cc, z_of(dz), at], sibling, f1.at[dz, ro], s1.at[par, dz, ro])

    near = [(0, 1), (0, 3), (1, 0), (0, 2)]
    far = [(1, 1), (1, 3), (1, 2)]
    pieces = [(0, 0)] + near + far

    def local(src, dst, n):
        return pltpu.make_async_copy(src, dst, w_sem.at[n])

    def qkv_copies(ref, at):
        cols = lambda part: pl.ds(pl.multiple_of(part * width + core * half_w, 128), half_w)
        return [local(ref.at[(*at, slice(None), cols(p))], w_qkv.at[:, pl.ds(p * half_w, half_w)], p) for p in range(3)]

    def proj_copies(ref, at):
        return [local(ref.at[at], w_proj, 3)]

    def up_copies(ref, at):
        return [local(ref.at[at], w_up, 4)]

    def down_copies(ref, at):
        return [local(ref.at[at], w_down, 5)]

    def skip_copies(j):
        return [local(skip_hbm.at[j], w_skip, 6)]

    def square(ref):
        return [local(ref, w_sq, 7)]

    def start(copies):
        for c in copies:
            c.start()

    def wait(copies):
        for c in copies:
            c.wait()

    kinds = (qkv_copies, proj_copies, up_copies, down_copies)
    in_refs, out_refs = (in_qkv, in_proj, in_up, in_down), (out_qkv, out_proj, out_up, out_down)
    lane = lax.broadcasted_iota(jnp.int32, (2 * ROWS, 128), 1)

    def block(par, norm, copies, start_next, beside):
        t_all[par, core, z_pos, r_pos, d_pos] = layer_norm(u_buf[...], norm[0:1, :], norm[1:2, :])
        for key in near:
            leg1(par, *key).start()
        for way in (0, 1):
            leg2(par, 0, 0, way).start()
        for key in far:
            leg1(par, *key).start()
        beside(0)
        for key in near + far:
            leg1(par, *key, receive=True).wait_recv()
            for way in ((2, 0, 1) if key == (1, 2) else (0, 1)):
                leg2(par, *key, way).start()
        for dz in (0, 1):
            side(par, dz, 0, core).start()
        beside(1)

        seen = {}

        def take(dz, d, way):
            leg2(par, dz, d, way, receive=True).wait_recv()
            if way == onward(dz, d) and (dz, d) != (1, 2):
                leg2(par, dz, d, 2).start()
            seen[dz, way] = seen.get((dz, way), 0) + 1
            if seen[dz, way] == 4:
                side(par, dz, (3, 1, 2)[way], core).start()

        def take_both(keys):
            for key in keys:
                take(*key, onward(*key))
                take(*key, 1 - onward(*key))

        def chunk(j, cc, ro):
            at = shift(r_pos if cc is core else d_pos, ro)
            toks = jnp.concatenate([t_all[par, cc, zz, at, o] for zz in range(2) for o in range(4)], axis=0)
            n = toks.shape[0]
            kv = mat_f32(toks, w_qkv[:, half_w:3 * half_w]).astype(jnp.bfloat16)
            v_buf[j * n:(j + 1) * n, :] = kv[:, half_w:]
            for p in range(3):
                sc = lax.dot_general(q_bd[p], kv[:, p * 128:(p + 1) * 128], (((1,), (1,)), ((), ())), preferred_element_type=jnp.float32)
                top = jnp.max(sc, axis=-1, keepdims=True)
                if j:
                    old = top_buf[p, j - 1]
                    top = jnp.maximum(old, top)
                e = jnp.exp2((sc - top) * SCALE)
                s_buf[p, :, j * n:(j + 1) * n] = e
                part = e[:, 0:128] + e[:, 128:256]
                sum_buf[p] = sum_buf[p] * jnp.exp2((old - top) * SCALE) + part if j else part
                top_buf[p, j] = top

        take_both(pieces[0:4])
        wait(copies(0))
        for dz in (0, 1):
            side(par, dz, 0, sib_core).wait_recv()
        own = jnp.concatenate([t_all[par, 0, z_pos, y_pos, x_pos], t_all[par, 1, z_pos, x_pos, y_pos]], axis=0)
        q = mat_f32(own, w_qkv[:, 0:half_w])
        q_bd = []
        for p in range(3):
            qp = q[:, p * 128:(p + 1) * 128]
            q_bd.append(jnp.concatenate([jnp.where(lane < 64, qp, 0.0), jnp.where(lane < 64, 0.0, qp)], axis=0).astype(jnp.bfloat16))
        chunk(0, core, 0)
        take_both(pieces[4:6])
        chunk(1, sib_core, 0)
        take_both(pieces[6:8])
        chunk(2, core, 3)
        chunk(3, core, 1)
        for key in pieces:
            take(*key, 2)
        for j, ro in ((4, 3), (5, 1)):
            for dz in (0, 1):
                side(par, dz, ro, sib_core).wait_recv()
            chunk(j, sib_core, ro)
        chunk(6, core, 2)
        for dz in (0, 1):
            side(par, dz, 2, sib_core).wait_recv()
        chunk(7, sib_core, 2)
        start_next(0)

        n_chunks, n = 8, 256
        for p in range(3):
            top = top_buf[p, n_chunks - 1]
            inv = 1.0 / jnp.sum(sum_buf[p], axis=-1, keepdims=True)
            acc = None
            for j in range(n_chunks):
                fac = inv if j == n_chunks - 1 else jnp.exp2((top_buf[p, j] - top) * SCALE) * inv
                pr = (s_buf[p, :, j * n:(j + 1) * n] * fac).astype(jnp.bfloat16)
                o = mat_f32(pr, v_buf[j * n:(j + 1) * n, p * 128:(p + 1) * 128])
                acc = o if acc is None else acc + o
            a = jnp.where(lane < 64, acc[0:2 * ROWS], acc[2 * ROWS:4 * ROWS]).astype(jnp.bfloat16)
            a_buf[0, :, p * 128:(p + 1) * 128] = a[0:ROWS]
            a_buf[1, :, p * 128:(p + 1) * 128] = a[ROWS:2 * ROWS]

        swap = send(a_buf.at[sib_core], a_full.at[core], sibling, a_send, a_recv)
        swap.start()
        a_full[core] = a_buf[core]
        swap.wait_send()
        send(a_buf.at[core], a_full.at[sib_core], sibling, a_send, a_recv).wait_recv()

        wait(copies(1))
        attn = mat_f32(a_full[0], w_proj[0:half_w, :]) + mat_f32(a_full[1], w_proj[half_w:width, :])
        start_next(1)
        mid = (u_buf[...].astype(jnp.float32) + attn).astype(jnp.bfloat16)
        t2 = layer_norm(mid, norm[2:3, :], norm[3:4, :])
        wait(copies(2))
        wait(copies(3))
        acc = None
        for c in range(0, hid, width):
            h = gelu(mat_f32(t2, w_up[:, c:c + width])).astype(jnp.bfloat16)
            o = mat_f32(h, w_down[c:c + width, :])
            acc = o if acc is None else acc + o
        start_next(2)
        start_next(3)
        u_buf[...] = (mid.astype(jnp.float32) + acc).astype(jnp.bfloat16)

        for dz in (0, 1):
            for d in range(4):
                if dz or d:
                    leg1(par, dz, d).wait_send()
                for way in range(3):
                    leg2(par, dz, d, way).wait_send()
            for ro in range(4):
                side(par, dz, ro, core).wait_send()

    start(square(hint_hbm))
    for make, ref in zip(kinds, in_refs):
        start(make(ref, (half, 0)))
    start(skip_copies(0))

    def swap_in(n, src):
        return send(src, xh_buf.at[n, half], partner, x_send.at[n], x_recv.at[n])

    for n, ref in enumerate((x_ref, hint_ref)):
        swap_in(n, ref).start()
        xh_buf[n, half] = ref[...]
    for n, ref in enumerate((x_ref, hint_ref)):
        swap_in(n, ref).wait_send()
        send(ref, xh_buf.at[n, 1 - half], partner, x_send.at[n], x_recv.at[n]).wait_recv()

    @pl.when(half == 1)
    def _():
        r_in[...] = jnp.zeros_like(r_in)

    x_loc = jnp.concatenate([xh_buf[0, 0], xh_buf[0, 1]], axis=0)
    hint_loc = jnp.concatenate([xh_buf[1, 0], xh_buf[1, 1]], axis=0)
    wait(square(hint_hbm))
    hinted = (x_loc.astype(jnp.float32) + mat_f32(hint_loc, w_sq[...])).astype(jnp.bfloat16)
    start(square(zero_hbm.at[0]))
    u_buf[...] = x_loc

    @pl.when(half == 1)
    def _():
        u_buf[...] = hinted

    def residual(i):
        wait(square(zero_hbm.at[i]))
        r_out[...] = mat_f32(u_buf[...], w_sq[...]).astype(jnp.bfloat16)

    def residual_copy(i):
        return send(r_out, r_in.at[i], partner, r_send, r_recv.at[i])

    def in_block(i, carry):
        copies = lambda n: kinds[n](in_refs[n], (half, i))

        def start_next(n):
            @pl.when(i + 1 < n_in)
            def _():
                start(kinds[n](in_refs[n], (half, i + 1)))

            @pl.when(i + 1 == n_in)
            def _():
                start(kinds[n](out_refs[n], (0,)))

        def beside(when):
            @pl.when(i > 0)
            def _():
                if when == 0:
                    residual(i - 1)
                    start(square(zero_hbm.at[i]))
                else:
                    @pl.when(half == 1)
                    def _():
                        residual_copy(i - 1).start()

        block(lax.rem(i, 2), in_norm.at[half, i], copies, start_next, beside)
        hist[i] = u_buf[...]

        @pl.when(jnp.logical_and(i > 0, half == 1))
        def _():
            residual_copy(i - 1).wait_send()

        return carry

    lax.fori_loop(0, n_in, in_block, 0)
    residual(n_in - 1)
    start(square(wout_hbm))

    @pl.when(half == 1)
    def _():
        residual_copy(n_in - 1).start()
        residual_copy(n_in - 1).wait_send()

    @pl.when(half == 0)
    def _():
        for i in range(n_in):
            residual_copy(i).wait_recv()

    def with_residual(i):
        return (hist[i].astype(jnp.float32) + r_in[i].astype(jnp.float32)).astype(jnp.bfloat16)

    u_buf[...] = with_residual(n_in - 1)

    def out_block(j, carry):
        copies = lambda n: kinds[n](out_refs[n], (j,))

        def start_next(n):
            @pl.when(j + 1 < n_out)
            def _():
                start(kinds[n](out_refs[n], (j + 1,)))

        wait(skip_copies(j))
        merged = mat_f32(u_buf[...], w_skip[0:width, :]) + mat_f32(with_residual(n_out - 1 - j), w_skip[width:2 * width, :])

        @pl.when(j + 1 < n_out)
        def _():
            start(skip_copies(j + 1))

        u_buf[...] = merged.astype(jnp.bfloat16)
        block(lax.rem(j + n_in, 2), out_norm.at[j], copies, start_next, lambda when: None)
        return carry

    lax.fori_loop(0, n_out, out_block, 0)

    normed = layer_norm(u_buf[...], final_norm[0:1, :], final_norm[1:2, :])
    wait(square(wout_hbm))
    y = mat_f32(normed, w_sq[...]).astype(jnp.bfloat16)
    y_out[0] = y[0:SLAB]
    y_out[1] = y[SLAB:ROWS]
    hand_over = send(y_out.at[1], y_in, partner, y_send, y_recv)

    @pl.when(half == 0)
    def _():
        hand_over.start()
        y_ref[...] = y_out[0]
        hand_over.wait_send()

    @pl.when(half == 1)
    def _():
        hand_over.wait_recv()
        y_ref[...] = y_in[...]


def solution(mesh):
    def device_step(x_own, hint_own, in_qkv, in_proj, in_up, in_down, in_norm, out_qkv, out_proj, out_up, out_down, out_norm, zero_proj, hint_proj, skip_proj, final_norm, w_out):
        width, hid, n_in = x_own.shape[-1], in_up.shape[-1], zero_proj.shape[0]
        vmem, hbm = pl.BlockSpec(memory_space=pltpu.VMEM), pl.BlockSpec(memory_space=pl.ANY)
        bf, f32, dma = jnp.bfloat16, jnp.float32, pltpu.SemaphoreType.DMA
        flat = lambda w: w.reshape(w.shape[:-3] + (width, width))
        scratch = [
            pltpu.VMEM((2, 2, 2, 4, 4, ROWS, width), bf),
            pltpu.VMEM((width, 3 * width // 2), bf), pltpu.VMEM((width, width), bf),
            pltpu.VMEM((width, hid), bf), pltpu.VMEM((hid, width), bf),
            pltpu.VMEM((2 * width, width), bf), pltpu.VMEM((width, width), bf),
            pltpu.VMEM((2048, width // 2), bf), pltpu.VMEM((3, 128, 2048), f32),
            pltpu.VMEM((3, 8, 128, 1), f32), pltpu.VMEM((3, 128, 128), f32),
            pltpu.VMEM((2, ROWS, width // 2), bf), pltpu.VMEM((2, ROWS, width // 2), bf),
            pltpu.VMEM((ROWS, width), bf), pltpu.VMEM((2, 2, SLAB, width), bf),
            pltpu.VMEM((n_in, ROWS, width), bf), pltpu.VMEM((ROWS, width), bf), pltpu.VMEM((n_in, ROWS, width), bf),
            pltpu.VMEM((2, SLAB, width), bf), pltpu.VMEM((SLAB, width), bf),
            dma((8,)),
            dma((2, 2, 4)), dma((2, 2, 4, 3)), dma((2, 2, 4)), dma((2, 4)), dma((2, 4, 3)), dma((2, 4)),
            dma(()), dma(()), dma((2,)), dma((2,)), dma((n_in,)), dma(()), dma(()), dma(()),
        ]
        return pl.pallas_call(
            net_kernel,
            out_shape=jax.ShapeDtypeStruct(x_own.shape, bf), in_specs=[vmem] * 5 + [hbm] * 12, out_specs=vmem,
            scratch_shapes=scratch, name="net",
            compiler_params=pltpu.CompilerParams(has_side_effects=True, vmem_limit_bytes=52 * 1024 * 1024),
        )(x_own, hint_own, in_norm.astype(f32), out_norm.astype(f32), final_norm.astype(f32), in_qkv, flat(in_proj), in_up, in_down,
          out_qkv, flat(out_proj), out_up, out_down, zero_proj, hint_proj, skip_proj, w_out)

    tok_spec = P(("data", "group"), None)
    return jax.shard_map(device_step, mesh=mesh, in_specs=(tok_spec, tok_spec) + (P(),) * 15, out_specs=tok_spec, check_vma=False)
```

```python
import functools

import jax
import jax.numpy as jnp
from jax import lax
from jax.experimental import pallas as pl
from jax.experimental.pallas import tpu as pltpu
from jax.sharding import PartitionSpec as P

EPS = 1e-6
MESH = pl.DeviceIdType.MESH
SCALE = 64 ** -0.5 * 1.4426950408889634
ROWS = 32
SLAB = 16


def mat_f32(left_op, right_op):
    return jnp.dot(left_op, right_op, preferred_element_type=jnp.float32)


def layer_norm(values, gain, shift):
    wide_vals = values.astype(jnp.float32)
    centered = wide_vals - jnp.mean(wide_vals, axis=-1, keepdims=True)
    variance = jnp.mean(centered * centered, axis=-1, keepdims=True)
    normed = centered * lax.rsqrt(variance + EPS)
    return (normed * gain + shift).astype(jnp.bfloat16)


def gelu(v):
    inner = 0.7978845608028654 * (v + 0.044715 * (v * v * v))
    return 0.5 * v * (1.0 + jnp.tanh(inner))


def net_kernel(x_ref, hint_ref, in_norm, out_norm, final_norm, in_qkv, in_proj, in_up, in_down,
               out_qkv, out_proj, out_up, out_down, zero_hbm, hint_hbm, skip_hbm, wout_hbm, y_ref,
               t_all, w_qkv, w_proj, w_up, w_down, w_skip, w_sq, v_buf, s_buf, top_buf, a_buf, a_full,
               u_buf, xh_buf, hist, r_out, r_in, y_out, y_in,
               w_sem, p1, p2, s1, q1, q2, f1, a_recv, a_send, x_recv, x_send, r_recv, r_send, y_recv, y_send):
    n_in, n_out = in_norm.shape[1], out_norm.shape[0]
    width = x_ref.shape[-1]
    half_w = width // 2
    hid = w_up.shape[-1]

    data_idx = lax.axis_index("data")
    me = lax.axis_index("group")
    core = lax.rem(me, 2)
    chip = me // 2
    x_pos = lax.rem(chip, 4)
    y_pos = lax.rem(chip // 4, 4)
    z_full = chip // 16
    half = z_full // 2
    z_pos = lax.rem(z_full, 2)
    sib_core = 1 - core
    sibling = me + 1 - 2 * core
    partner = me + 64 - 128 * half
    r_pos = y_pos + core * (x_pos - y_pos)
    d_pos = x_pos + core * (y_pos - x_pos)

    def dev(zz, r, d):
        yy = r + core * (d - r)
        xx = d + core * (r - d)
        return (((half * 2 + zz) * 4 + yy) * 4 + xx) * 2 + core

    def shift(pos, d):
        return lax.rem(pos + d + 4, 4)

    def z_of(dz):
        return z_pos if dz == 0 else 1 - z_pos

    def send(src, dst, target, send_sem, recv_sem):
        return pltpu.make_async_remote_copy(
            src_ref=src, dst_ref=dst, send_sem=send_sem, recv_sem=recv_sem,
            device_id=(data_idx, target), device_id_type=MESH)

    def remote(region, target, send_sem, recv_sem):
        return send(region, region, target, send_sem, recv_sem)

    def leg1(par, dz, d, receive=False):
        sems = (q1.at[dz, d], p1.at[par, dz, d])
        if receive:
            return remote(t_all.at[par, core, z_of(dz), r_pos, shift(d_pos, -d)], sibling, *sems)
        return remote(t_all.at[par, core, z_pos, r_pos, d_pos], dev(z_of(dz), r_pos, shift(d_pos, d)), *sems)

    def onward(dz, d):
        return (dz + (d in (1, 2))) % 2

    def leg2(par, dz, d, way, receive=False):
        sems = (q2.at[dz, d, way], p2.at[par, dz, d, way])
        zz, dd = z_of(dz), shift(d_pos, -d)
        if way < 2:
            w = 1 - 2 * way
            at, to = (shift(r_pos, -w) if receive else r_pos), shift(r_pos, w)
        elif (dz, d) == (1, 2):
            at, to = (shift(r_pos, 2) if receive else r_pos), shift(r_pos, 2)
        else:
            w = 1 - 2 * onward(dz, d)
            at, to = shift(r_pos, 2 if receive else -w), shift(r_pos, w)
        return remote(t_all.at[par, core, zz, at, dd], dev(z_pos, to, d_pos), *sems)

    def side(par, dz, ro, cc):
        at = shift(r_pos if cc is core else d_pos, ro)
        return remote(t_all.at[par, cc, z_of(dz), at], sibling, f1.at[dz, ro], s1.at[par, dz, ro])

    near = [(0, 1), (0, 3), (1, 0), (0, 2)]
    far = [(1, 1), (1, 3), (1, 2)]
    pieces = [(0, 0)] + near + far

    def local(src, dst, n):
        return pltpu.make_async_copy(src, dst, w_sem.at[n])

    def qkv_copies(ref, at):
        cols = lambda part: pl.ds(pl.multiple_of(part * width + core * half_w, 128), half_w)
        return [local(ref.at[(*at, slice(None), cols(p))], w_qkv.at[:, pl.ds(p * half_w, half_w)], p) for p in range(3)]

    def proj_copies(ref, at):
        return [local(ref.at[at], w_proj, 3)]

    def up_copies(ref, at):
        return [local(ref.at[at], w_up, 4)]

    def down_copies(ref, at):
        return [local(ref.at[at], w_down, 5)]

    def skip_copies(j):
        return [local(skip_hbm.at[j], w_skip, 6)]

    def square(ref):
        return [local(ref, w_sq, 7)]

    def start(copies):
        for c in copies:
            c.start()

    def wait(copies):
        for c in copies:
            c.wait()

    kinds = (qkv_copies, proj_copies, up_copies, down_copies)
    in_refs, out_refs = (in_qkv, in_proj, in_up, in_down), (out_qkv, out_proj, out_up, out_down)
    lane = lax.broadcasted_iota(jnp.int32, (2 * ROWS, 128), 1)

    def block(par, norm, copies, start_next, beside):
        t_all[par, core, z_pos, r_pos, d_pos] = layer_norm(u_buf[...], norm[0:1, :], norm[1:2, :])
        for key in near:
            leg1(par, *key).start()
        for way in (0, 1):
            leg2(par, 0, 0, way).start()
        for key in far:
            leg1(par, *key).start()
        beside(0)
        for key in near + far:
            leg1(par, *key, receive=True).wait_recv()
            for way in ((2, 0, 1) if key == (1, 2) else (0, 1)):
                leg2(par, *key, way).start()
        for dz in (0, 1):
            side(par, dz, 0, core).start()
        beside(1)

        seen = {}

        def take(dz, d, way):
            leg2(par, dz, d, way, receive=True).wait_recv()
            if way == onward(dz, d) and (dz, d) != (1, 2):
                leg2(par, dz, d, 2).start()
            seen[dz, way] = seen.get((dz, way), 0) + 1
            if seen[dz, way] == 4:
                side(par, dz, (3, 1, 2)[way], core).start()

        def take_both(keys):
            for key in keys:
                take(*key, onward(*key))
                take(*key, 1 - onward(*key))

        def chunk(j, cc, ro):
            at = shift(r_pos if cc is core else d_pos, ro)
            toks = jnp.concatenate([t_all[par, cc, zz, at, o] for zz in range(2) for o in range(4)], axis=0)
            n = toks.shape[0]
            kv = mat_f32(toks, w_qkv[:, half_w:3 * half_w]).astype(jnp.bfloat16)
            v_buf[j * n:(j + 1) * n, :] = kv[:, half_w:]
            for p in range(3):
                sc = lax.dot_general(q_bd[p], kv[:, p * 128:(p + 1) * 128], (((1,), (1,)), ((), ())), preferred_element_type=jnp.float32)
                s_buf[p, :, j * n:(j + 1) * n] = sc
                top = jnp.maximum(sc[:, 0:128], sc[:, 128:256])
                top_buf[p] = jnp.maximum(top_buf[p], top) if j else top

        def side_in(ro):
            for dz in (0, 1):
                side(par, dz, ro, sib_core).wait_recv()

        take_both(pieces)
        wait(copies(0))
        side_in(0)
        own = jnp.concatenate([t_all[par, 0, z_pos, y_pos, x_pos], t_all[par, 1, z_pos, x_pos, y_pos]], axis=0)
        q = mat_f32(own, w_qkv[:, 0:half_w])
        q_bd = []
        for p in range(3):
            qp = q[:, p * 128:(p + 1) * 128]
            q_bd.append(jnp.concatenate([jnp.where(lane < 64, qp, 0.0), jnp.where(lane < 64, 0.0, qp)], axis=0).astype(jnp.bfloat16))
        chunk(0, core, 0)
        chunk(1, sib_core, 0)
        chunk(2, core, 3)
        chunk(3, core, 1)
        for key in pieces:
            take(*key, 2)
        side_in(3)
        chunk(4, sib_core, 3)
        side_in(1)
        chunk(5, sib_core, 1)
        chunk(6, core, 2)
        side_in(2)
        chunk(7, sib_core, 2)
        start_next(0)

        n_chunks, n = 8, 256
        for p in range(3):
            top = jnp.max(top_buf[p], axis=-1, keepdims=True)
            part = None
            for j in range(n_chunks):
                e = jnp.exp2((s_buf[p, :, j * n:(j + 1) * n] - top) * SCALE)
                s_buf[p, :, j * n:(j + 1) * n] = e
                both = e[:, 0:128] + e[:, 128:256]
                part = both if part is None else part + both
            inv = 1.0 / jnp.sum(part, axis=-1, keepdims=True)
            acc = None
            for j in range(n_chunks):
                pr = (s_buf[p, :, j * n:(j + 1) * n] * inv).astype(jnp.bfloat16)
                o = mat_f32(pr, v_buf[j * n:(j + 1) * n, p * 128:(p + 1) * 128])
                acc = o if acc is None else acc + o
            a = jnp.where(lane < 64, acc[0:2 * ROWS], acc[2 * ROWS:4 * ROWS]).astype(jnp.bfloat16)
            a_buf[0, :, p * 128:(p + 1) * 128] = a[0:ROWS]
            a_buf[1, :, p * 128:(p + 1) * 128] = a[ROWS:2 * ROWS]

        swap = send(a_buf.at[sib_core], a_full.at[core], sibling, a_send, a_recv)
        swap.start()
        a_full[core] = a_buf[core]
        swap.wait_send()
        send(a_buf.at[core], a_full.at[sib_core], sibling, a_send, a_recv).wait_recv()

        wait(copies(1))
        attn = mat_f32(a_full[0], w_proj[0:half_w, :]) + mat_f32(a_full[1], w_proj[half_w:width, :])
        start_next(1)
        mid = (u_buf[...].astype(jnp.float32) + attn).astype(jnp.bfloat16)
        t2 = layer_norm(mid, norm[2:3, :], norm[3:4, :])
        wait(copies(2))
        wait(copies(3))
        acc = None
        for c in range(0, hid, width):
            h = gelu(mat_f32(t2, w_up[:, c:c + width])).astype(jnp.bfloat16)
            o = mat_f32(h, w_down[c:c + width, :])
            acc = o if acc is None else acc + o
        start_next(2)
        start_next(3)
        u_buf[...] = (mid.astype(jnp.float32) + acc).astype(jnp.bfloat16)

        for dz in (0, 1):
            for d in range(4):
                if dz or d:
                    leg1(par, dz, d).wait_send()
                for way in range(3):
                    leg2(par, dz, d, way).wait_send()
            for ro in range(4):
                side(par, dz, ro, core).wait_send()

    start(square(hint_hbm))
    for make, ref in zip(kinds, in_refs):
        start(make(ref, (half, 0)))
    start(skip_copies(0))

    def swap_in(n, src):
        return send(src, xh_buf.at[n, half], partner, x_send.at[n], x_recv.at[n])

    for n, ref in enumerate((x_ref, hint_ref)):
        swap_in(n, ref).start()
        xh_buf[n, half] = ref[...]
    for n, ref in enumerate((x_ref, hint_ref)):
        swap_in(n, ref).wait_send()
        send(ref, xh_buf.at[n, 1 - half], partner, x_send.at[n], x_recv.at[n]).wait_recv()

    @pl.when(half == 1)
    def _():
        r_in[...] = jnp.zeros_like(r_in)

    x_loc = jnp.concatenate([xh_buf[0, 0], xh_buf[0, 1]], axis=0)
    hint_loc = jnp.concatenate([xh_buf[1, 0], xh_buf[1, 1]], axis=0)
    wait(square(hint_hbm))
    hinted = (x_loc.astype(jnp.float32) + mat_f32(hint_loc, w_sq[...])).astype(jnp.bfloat16)
    start(square(zero_hbm.at[0]))
    u_buf[...] = x_loc

    @pl.when(half == 1)
    def _():
        u_buf[...] = hinted

    def residual(i):
        wait(square(zero_hbm.at[i]))
        r_out[...] = mat_f32(u_buf[...], w_sq[...]).astype(jnp.bfloat16)

    def residual_copy(i):
        return send(r_out, r_in.at[i], partner, r_send, r_recv.at[i])

    def in_block(i, carry):
        copies = lambda n: kinds[n](in_refs[n], (half, i))

        def start_next(n):
            @pl.when(i + 1 < n_in)
            def _():
                start(kinds[n](in_refs[n], (half, i + 1)))

            @pl.when(i + 1 == n_in)
            def _():
                start(kinds[n](out_refs[n], (0,)))

        def beside(when):
            @pl.when(i > 0)
            def _():
                if when == 0:
                    residual(i - 1)
                    start(square(zero_hbm.at[i]))
                else:
                    @pl.when(half == 1)
                    def _():
                        residual_copy(i - 1).start()

        block(lax.rem(i, 2), in_norm.at[half, i], copies, start_next, beside)
        hist[i] = u_buf[...]

        @pl.when(jnp.logical_and(i > 0, half == 1))
        def _():
            residual_copy(i - 1).wait_send()

        return carry

    lax.fori_loop(0, n_in, in_block, 0)
    residual(n_in - 1)
    start(square(wout_hbm))

    @pl.when(half == 1)
    def _():
        residual_copy(n_in - 1).start()
        residual_copy(n_in - 1).wait_send()

    @pl.when(half == 0)
    def _():
        for i in range(n_in):
            residual_copy(i).wait_recv()

    def with_residual(i):
        return (hist[i].astype(jnp.float32) + r_in[i].astype(jnp.float32)).astype(jnp.bfloat16)

    u_buf[...] = with_residual(n_in - 1)

    def out_block(j, carry):
        copies = lambda n: kinds[n](out_refs[n], (j,))

        def start_next(n):
            @pl.when(j + 1 < n_out)
            def _():
                start(kinds[n](out_refs[n], (j + 1,)))

        wait(skip_copies(j))
        merged = mat_f32(u_buf[...], w_skip[0:width, :]) + mat_f32(with_residual(n_out - 1 - j), w_skip[width:2 * width, :])

        @pl.when(j + 1 < n_out)
        def _():
            start(skip_copies(j + 1))

        u_buf[...] = merged.astype(jnp.bfloat16)
        block(lax.rem(j + n_in, 2), out_norm.at[j], copies, start_next, lambda when: None)
        return carry

    lax.fori_loop(0, n_out, out_block, 0)

    normed = layer_norm(u_buf[...], final_norm[0:1, :], final_norm[1:2, :])
    wait(square(wout_hbm))
    y = mat_f32(normed, w_sq[...]).astype(jnp.bfloat16)
    y_out[0] = y[0:SLAB]
    y_out[1] = y[SLAB:ROWS]
    hand_over = send(y_out.at[1], y_in, partner, y_send, y_recv)

    @pl.when(half == 0)
    def _():
        hand_over.start()
        y_ref[...] = y_out[0]
        hand_over.wait_send()

    @pl.when(half == 1)
    def _():
        hand_over.wait_recv()
        y_ref[...] = y_in[...]


def solution(mesh):
    def device_step(x_own, hint_own, in_qkv, in_proj, in_up, in_down, in_norm, out_qkv, out_proj, out_up, out_down, out_norm, zero_proj, hint_proj, skip_proj, final_norm, w_out):
        width, hid, n_in = x_own.shape[-1], in_up.shape[-1], zero_proj.shape[0]
        vmem, hbm = pl.BlockSpec(memory_space=pltpu.VMEM), pl.BlockSpec(memory_space=pl.ANY)
        bf, f32, dma = jnp.bfloat16, jnp.float32, pltpu.SemaphoreType.DMA
        flat = lambda w: w.reshape(w.shape[:-3] + (width, width))
        scratch = [
            pltpu.VMEM((2, 2, 2, 4, 4, ROWS, width), bf),
            pltpu.VMEM((width, 3 * width // 2), bf), pltpu.VMEM((width, width), bf),
            pltpu.VMEM((width, hid), bf), pltpu.VMEM((hid, width), bf),
            pltpu.VMEM((2 * width, width), bf), pltpu.VMEM((width, width), bf),
            pltpu.VMEM((2048, width // 2), bf), pltpu.VMEM((3, 128, 2048), f32),
            pltpu.VMEM((3, 128, 128), f32),
            pltpu.VMEM((2, ROWS, width // 2), bf), pltpu.VMEM((2, ROWS, width // 2), bf),
            pltpu.VMEM((ROWS, width), bf), pltpu.VMEM((2, 2, SLAB, width), bf),
            pltpu.VMEM((n_in, ROWS, width), bf), pltpu.VMEM((ROWS, width), bf), pltpu.VMEM((n_in, ROWS, width), bf),
            pltpu.VMEM((2, SLAB, width), bf), pltpu.VMEM((SLAB, width), bf),
            dma((8,)),
            dma((2, 2, 4)), dma((2, 2, 4, 3)), dma((2, 2, 4)), dma((2, 4)), dma((2, 4, 3)), dma((2, 4)),
            dma(()), dma(()), dma((2,)), dma((2,)), dma((n_in,)), dma(()), dma(()), dma(()),
        ]
        return pl.pallas_call(
            net_kernel,
            out_shape=jax.ShapeDtypeStruct(x_own.shape, bf), in_specs=[vmem] * 5 + [hbm] * 12, out_specs=vmem,
            scratch_shapes=scratch, name="net",
            compiler_params=pltpu.CompilerParams(has_side_effects=True, vmem_limit_bytes=52 * 1024 * 1024),
        )(x_own, hint_own, in_norm.astype(f32), out_norm.astype(f32), final_norm.astype(f32), in_qkv, flat(in_proj), in_up, in_down,
          out_qkv, flat(out_proj), out_up, out_down, zero_proj, hint_proj, skip_proj, w_out)

    tok_spec = P(("data", "group"), None)
    return jax.shard_map(device_step, mesh=mesh, in_specs=(tok_spec, tok_spec) + (P(),) * 15, out_specs=tok_spec, check_vma=False)
```
